32 devices in a mesh: row: 8 (over z, y), col: 4 (over x, core).
Axes of the slice: x: 2, y: 2, z: 4, core: 2. Of those that a mesh axis runs over, the one named last changes fastest.
Arguments:
- features: float32 [32, 3072], P(None, ('row', 'col')), may hold values from -6 to 6
- block: float32 [16, 3072], P(None, ('row', 'col')), may hold values from -6 to 6
Outputs:
- applied: float32 [16, 3072], P(None, ('row', 'col'))
The draws below stay inside these ranges and needn't reach their ends.
All inputs are finite; a program needn't handle non-finite values.
Results may differ from the reference program's by a relative error of at most 0.006.
Values may be sent and summed in bfloat16 or wider, within the bound.
A program may use at most 64 MiB of HBM per device.

```python
import math
import jax
import jax.numpy as jnp
from jax import lax

F = 32
BLOCK = 16
FRAMES = 3072


def level_of(own_key, dims, cuts, smallest, high):
    loudness, own = 1.0, jax.random.fold_in(own_key, 6)
    for dim, blocks in cuts:
        draws = jnp.exp(jax.random.uniform(jax.random.fold_in(own, dim), (blocks,), jnp.float32, smallest / len(cuts), high / len(cuts)))
        loudness = loudness * jnp.repeat(draws, dims[dim] // blocks).reshape([-1 if axis == dim else 1 for axis in range(len(dims))])
    return loudness


def normal_values(stream_key, extent, deviation, reach, cuts=(), kind=jnp.bfloat16):
    result = deviation * jax.random.normal(stream_key, extent, jnp.float32)
    if cuts:
        result = result * level_of(stream_key, extent, cuts, -0.22, 0.18)
    return jnp.clip(result, -reach, reach).astype(kind)


def setup_inputs(seed: int = 0) -> dict:
    seeds = jax.random.split(jax.random.key(seed), 3)
    return {
        "features": normal_values(seeds[0], (F, FRAMES), 1.0, 6.0, ((1, 32),), jnp.float32),
        "block": normal_values(seeds[1], (BLOCK, FRAMES), 1.0, 6.0, ((1, 32),), jnp.float32),
    }


def kernel_rows(row_feat, row_sq, col_feat, col_sq, scale, start, count):
    part = lax.dynamic_slice_in_dim(row_feat, start, count, 1)
    sq_part = lax.dynamic_slice_in_dim(row_sq, start, count, 0)
    inner = jnp.einsum('fi,fj->ij', part, col_feat, precision=lax.Precision.HIGHEST)
    dist = sq_part[:, None] + col_sq[None, :] - 2.0 * inner
    return jnp.exp(-dist / scale).astype(jnp.bfloat16)

def reference(features, block):
    scale = 4.0 / (float(FRAMES) ** (2.0 / F) - 1.0)
    sq = lax.optimization_barrier(jnp.sum(features * features, axis=0))
    step = math.gcd(512, FRAMES)
    starts = jnp.arange(FRAMES // step, dtype=jnp.int32) * step

    def tile(start):
        return kernel_rows(features, sq, features, sq, scale, start, step)
    q = lax.map(lambda s: lax.optimization_barrier(jnp.sum(tile(s), axis=1, dtype=jnp.float32)), starts).reshape(-1)
    inv_q = 1.0 / q
    second = lax.map(lambda s: lax.optimization_barrier(jnp.sum(tile(s).astype(jnp.float32) * inv_q[None, :], axis=1)), starts).reshape(-1)
    dens = second * inv_q
    factor = inv_q * lax.rsqrt(dens)
    weighted = (block * factor[None, :]).astype(jnp.bfloat16)
    parts = lax.map(lambda s: jnp.dot(tile(s), weighted.T, preferred_element_type=jnp.float32), starts)
    summed = parts.reshape(FRAMES, BLOCK).T
    return summed * factor[None, :]
```

```python
import math

import jax
import jax.numpy as jnp
from jax import lax
from jax.experimental import pallas as pl
from jax.experimental.pallas import tpu as pltpu
from jax.sharding import PartitionSpec as P

F32 = jnp.float32
BF16 = jnp.bfloat16


def split(value, pieces):
    out = []
    for _ in range(pieces):
        piece = value.astype(BF16).astype(F32)
        out.append(piece)
        value = value - piece
    return out


def body(
    n_a, n_b, n_y, n_col, root,
    feat_ref, block_ref, out_ref,
    pad_ref, u_ref, v_ref, blk_ref, kern_ref, csum_ref, rsum_ref, sec_ref, part_ref, got_ref, fac_ref,
    u_s, u_r, v_s, v_r, k_s, k_r, c_s, c_r, r_s, r_r, s_s, s_r, p_s, p_r,
):
    width, owned = feat_ref.shape
    row, col = lax.axis_index("row"), lax.axis_index("col")
    a = row // n_y
    b = (row % n_y) * n_col + col
    a_peers = [lax.rem(a + k, n_a) for k in range(1, n_a)]
    b_peers = [lax.rem(b + k, n_b) for k in range(1, n_b)]

    def a_dev(peer):
        return (peer * n_y + b // n_col, b % n_col)

    def b_dev(peer):
        return (a * n_y + peer // n_col, peer % n_col)

    def copy(src, dst, send, recv, dev):
        return pltpu.make_async_remote_copy(
            src_ref=src, dst_ref=dst, send_sem=send, recv_sem=recv,
            device_id=dev, device_id_type=pl.DeviceIdType.MESH,
        )

    barrier = pltpu.get_barrier_semaphore()
    for peer in a_peers:
        pl.semaphore_signal(barrier, inc=1, device_id=a_dev(peer), device_id_type=pl.DeviceIdType.MESH)
    for peer in b_peers:
        pl.semaphore_signal(barrier, inc=1, device_id=b_dev(peer), device_id_type=pl.DeviceIdType.MESH)

    pad_ref[...] = jnp.zeros_like(pad_ref)
    pad_ref[:, :owned] = feat_ref[...] * root
    hi, lo = split(pad_ref[...], 2)
    half = jnp.sum(hi * (0.5 * hi + lo), axis=0, keepdims=True)
    t = [-piece for piece in split(half, 3)]
    one = jnp.ones_like(half)
    zero = jnp.zeros((128 - 3 * width - 6, pad_ref.shape[1]), F32)
    left = jnp.concatenate([hi, lo, hi] + t + [one] * 3 + [zero], axis=0)
    right = jnp.concatenate([hi, hi, lo] + [one] * 3 + t + [zero], axis=0)
    u_ref[b] = left.T[:owned].astype(BF16)
    v_ref[a] = right.T[:owned].astype(BF16)
    blk_ref[b] = block_ref[...]

    pl.semaphore_wait(barrier, n_a + n_b - 2)

    sends = []

    def send(cp):
        cp.start()
        sends.append(cp)

    for k, peer in enumerate(a_peers):
        send(copy(v_ref.at[a], v_ref.at[a], v_s.at[k], v_r.at[a], a_dev(peer)))
    for k, peer in enumerate(b_peers):
        send(copy(u_ref.at[b], u_ref.at[b], u_s.at[k], u_r.at[b], b_dev(peer)))
    for k, peer in enumerate(b_peers):
        send(copy(block_ref, blk_ref.at[b], k_s.at[k], k_r.at[b], b_dev(peer)))

    for peer in a_peers:
        copy(v_ref.at[a], v_ref.at[peer], v_s.at[0], v_r.at[peer], a_dev(peer)).wait_recv()
    v = v_ref[...].reshape(n_a * owned, 128)

    total = jnp.zeros((8, n_a * owned), F32)
    for peer in [b] + b_peers:
        if peer is not b:
            copy(u_ref.at[b], u_ref.at[peer], u_s.at[0], u_r.at[peer], b_dev(peer)).wait_recv()
        expo = lax.dot_general(u_ref[peer], v, (((1,), (1,)), ((), ())), preferred_element_type=F32)
        tile = jnp.exp2(expo).astype(BF16)
        kern_ref[peer] = tile
        total = total + jnp.sum(tile.astype(F32).reshape(owned // 8, 8, n_a * owned), axis=0)

    csum_ref[a] = jnp.sum(total, axis=0, keepdims=True)
    for k, peer in enumerate(a_peers):
        send(copy(csum_ref.at[a], csum_ref.at[a], c_s.at[k], c_r.at[a], a_dev(peer)))

    kern = kern_ref[...].reshape(n_b * owned, n_a * owned)
    nt = (((1,), (1,)), ((), ()))
    ones = jnp.ones((16, n_a * owned), BF16)
    rsum_ref[b] = lax.dot_general(ones, kern, nt, preferred_element_type=F32)[:1]
    for k, peer in enumerate(b_peers):
        send(copy(rsum_ref.at[b], rsum_ref.at[b], r_s.at[k], r_r.at[b], b_dev(peer)))

    for peer in b_peers:
        copy(block_ref, blk_ref.at[peer], k_s.at[0], k_r.at[peer], b_dev(peer)).wait_recv()
    blocks = jnp.concatenate([blk_ref[i] for i in range(n_b)], axis=1)

    for peer in a_peers:
        copy(csum_ref.at[a], csum_ref.at[peer], c_s.at[0], c_r.at[peer], a_dev(peer)).wait_recv()
    inv_c = 1.0 / jnp.sum(csum_ref[...], axis=0)
    lhs = jnp.concatenate(split(inv_c, 3) + [jnp.zeros((13, n_a * owned), F32)], axis=0).astype(BF16)
    sec = lax.dot_general(lhs, kern, nt, preferred_element_type=F32)
    sec_ref[b] = sec[0:1] + sec[1:2] + sec[2:3]
    for k, peer in enumerate(b_peers):
        send(copy(sec_ref.at[b], sec_ref.at[b], s_s.at[k], s_r.at[b], b_dev(peer)))

    for peer in b_peers:
        copy(rsum_ref.at[b], rsum_ref.at[peer], r_s.at[0], r_r.at[peer], b_dev(peer)).wait_recv()
    inv_r = 1.0 / jnp.sum(rsum_ref[...], axis=0)
    for peer in b_peers:
        copy(sec_ref.at[b], sec_ref.at[peer], s_s.at[0], s_r.at[peer], b_dev(peer)).wait_recv()
    dens = jnp.sum(sec_ref[...], axis=0) * inv_r
    factor = inv_r * lax.rsqrt(dens)
    for i in range(n_b):
        fac_ref[i] = factor[:, i * owned:(i + 1) * owned]
    weighted = (blocks * factor).astype(BF16)
    partial = jnp.dot(weighted, kern, preferred_element_type=F32)
    for i in range(n_a):
        part_ref[i] = partial[:, i * owned:(i + 1) * owned]
    for k, peer in enumerate(a_peers):
        send(copy(part_ref.at[peer], got_ref.at[a], p_s.at[k], p_r.at[a], a_dev(peer)))
    got_ref[a] = part_ref[a]
    for peer in a_peers:
        copy(part_ref.at[a], got_ref.at[peer], p_s.at[0], p_r.at[peer], a_dev(peer)).wait_recv()
    out_ref[...] = jnp.sum(got_ref[...], axis=0) * fac_ref[b]
    for cp in sends:
        cp.wait_send()


def per_device(features, block):
    n_row = lax.axis_size("row")
    n_col = lax.axis_size("col")
    n_y = 2 if n_row % 2 == 0 else 1
    n_a, n_b = n_row // n_y, n_y * n_col
    width, owned = features.shape
    columns = block.shape[0]
    frames = owned * n_row * n_col
    scale = 4.0 / (float(frames) ** (2.0 / width) - 1.0)
    root = math.sqrt(2.0 * math.log2(math.e) / scale)
    lanes = 128 * ((owned + 127) // 128)
    dma = pltpu.SemaphoreType.DMA
    a_sem, b_sem = dma((n_a,)), dma((n_b,))

    def kernel(*refs):
        body(n_a, n_b, n_y, n_col, root, *refs)

    vmem = pl.BlockSpec(memory_space=pltpu.VMEM)
    return pl.pallas_call(
        kernel,
        out_shape=jax.ShapeDtypeStruct(block.shape, F32),
        in_specs=[vmem, vmem],
        out_specs=vmem,
        scratch_shapes=[
            pltpu.VMEM((width, lanes), F32),
            pltpu.VMEM((n_b, owned, 128), BF16),
            pltpu.VMEM((n_a, owned, 128), BF16),
            pltpu.VMEM((n_b, columns, owned), F32),
            pltpu.VMEM((n_b, owned, n_a * owned), BF16),
            pltpu.VMEM((n_a, 1, n_a * owned), F32),
            pltpu.VMEM((n_b, 1, n_b * owned), F32),
            pltpu.VMEM((n_b, 1, n_b * owned), F32),
            pltpu.VMEM((n_a, columns, owned), F32),
            pltpu.VMEM((n_a, columns, owned), F32),
            pltpu.VMEM((n_b, 1, owned), F32),
            b_sem, b_sem, a_sem, a_sem, b_sem, b_sem, a_sem, a_sem,
            b_sem, b_sem, b_sem, b_sem, a_sem, a_sem,
        ],
        compiler_params=pltpu.CompilerParams(collective_id=0, has_side_effects=True),
        name="diffusion",
    )(features, block)


def solution(mesh):
    placed = (P(None, ("row", "col")), P(None, ("row", "col")))
    return jax.shard_map(
        per_device, mesh=mesh, in_specs=placed, out_specs=P(None, ("row", "col")), check_vma=False
    )
```

```python
import math

import jax
import jax.numpy as jnp
from jax import lax
from jax.experimental import pallas as pl
from jax.experimental.pallas import tpu as pltpu
from jax.sharding import PartitionSpec as P

F32 = jnp.float32
BF16 = jnp.bfloat16


def split(value, pieces):
    out = []
    for _ in range(pieces):
        piece = value.astype(BF16).astype(F32)
        out.append(piece)
        value = value - piece
    return out


def body(
    n_a, n_b, n_y, n_col, root,
    feat_hbm, block_hbm, out_ref,
    feat_ref, pad_ref, u_ref, v_ref, blk_ref, kern_ref, csum_ref, rsum_ref, sec_ref, part_ref, got_ref, fac_ref,
    f_l, k_l, u_s, u_r, v_s, v_r, k_s, k_r, c_s, c_r, r_s, r_r, s_s, s_r, p_s, p_r,
):
    width, owned = feat_ref.shape
    row, col = lax.axis_index("row"), lax.axis_index("col")
    a = (row % n_y) * n_col + col
    b = row // n_y
    a_peers = [lax.rem(a + k, n_a) for k in range(1, n_a)]
    b_peers = [lax.rem(b + k, n_b) for k in range(1, n_b)]

    def a_dev(peer):
        return (b * n_y + peer // n_col, peer % n_col)

    def b_dev(peer):
        return (peer * n_y + row % n_y, col)

    def copy(src, dst, send, recv, dev):
        return pltpu.make_async_remote_copy(
            src_ref=src, dst_ref=dst, send_sem=send, recv_sem=recv,
            device_id=dev, device_id_type=pl.DeviceIdType.MESH,
        )

    barrier = pltpu.get_barrier_semaphore()
    for peer in a_peers:
        pl.semaphore_signal(barrier, inc=1, device_id=a_dev(peer), device_id_type=pl.DeviceIdType.MESH)
    for peer in b_peers:
        pl.semaphore_signal(barrier, inc=1, device_id=b_dev(peer), device_id_type=pl.DeviceIdType.MESH)

    load = pltpu.make_async_copy(feat_hbm, feat_ref, f_l)
    load.start()
    load_block = pltpu.make_async_copy(block_hbm, blk_ref.at[b], k_l)
    load_block.start()
    pad_ref[...] = jnp.zeros_like(pad_ref)
    load.wait()
    pad_ref[:, :owned] = feat_ref[...] * root
    hi, lo = split(pad_ref[...], 2)
    half = jnp.sum(hi * (0.5 * hi + lo), axis=0, keepdims=True)
    t = [-piece for piece in split(half, 3)]
    one = jnp.ones_like(half)
    zero = jnp.zeros((128 - 3 * width - 6, pad_ref.shape[1]), F32)
    left = jnp.concatenate([hi, lo, hi] + t + [one] * 3 + [zero], axis=0)
    right = jnp.concatenate([hi, hi, lo] + [one] * 3 + t + [zero], axis=0)
    u_ref[b] = left.T[:owned].astype(BF16)
    v_ref[a] = right.T[:owned].astype(BF16)

    pl.semaphore_wait(barrier, n_a + n_b - 2)

    sends = []

    def send(cp):
        cp.start()
        sends.append(cp)

    for k, peer in enumerate(a_peers):
        send(copy(v_ref.at[a], v_ref.at[a], v_s.at[k], v_r.at[a], a_dev(peer)))
    for k, peer in enumerate(b_peers):
        send(copy(u_ref.at[b], u_ref.at[b], u_s.at[k], u_r.at[b], b_dev(peer)))
    for k, peer in enumerate(b_peers):
        if k == 0:
            load_block.wait()
        send(copy(blk_ref.at[b], blk_ref.at[b], k_s.at[k], k_r.at[b], b_dev(peer)))

    for peer in a_peers:
        copy(v_ref.at[a], v_ref.at[peer], v_s.at[0], v_r.at[peer], a_dev(peer)).wait_recv()
    v = v_ref[...].reshape(n_a * owned, 128)

    total = jnp.zeros((8, n_a * owned), F32)
    for peer in [b] + b_peers:
        if peer is not b:
            copy(u_ref.at[b], u_ref.at[peer], u_s.at[0], u_r.at[peer], b_dev(peer)).wait_recv()
        expo = lax.dot_general(u_ref[peer], v, (((1,), (1,)), ((), ())), preferred_element_type=F32)
        tile = jnp.exp2(expo).astype(BF16)
        kern_ref[peer] = tile
        total = total + jnp.sum(tile.astype(F32).reshape(owned // 8, 8, n_a * owned), axis=0)

    csum_ref[a] = jnp.sum(total, axis=0, keepdims=True)
    for k, peer in enumerate(a_peers):
        send(copy(csum_ref.at[a], csum_ref.at[a], c_s.at[k], c_r.at[a], a_dev(peer)))

    kern = kern_ref[...].reshape(n_b * owned, n_a * owned)
    nt = (((1,), (1,)), ((), ()))
    ones = jnp.ones((16, n_a * owned), BF16)
    rsum_ref[b] = lax.dot_general(ones, kern, nt, preferred_element_type=F32)[:1]
    for k, peer in enumerate(b_peers):
        send(copy(rsum_ref.at[b], rsum_ref.at[b], r_s.at[k], r_r.at[b], b_dev(peer)))

    for peer in b_peers:
        copy(blk_ref.at[b], blk_ref.at[peer], k_s.at[0], k_r.at[peer], b_dev(peer)).wait_recv()
    blocks = jnp.concatenate([blk_ref[i] for i in range(n_b)], axis=1)

    for peer in a_peers:
        copy(csum_ref.at[a], csum_ref.at[peer], c_s.at[0], c_r.at[peer], a_dev(peer)).wait_recv()
    inv_c = 1.0 / jnp.sum(csum_ref[...], axis=0)
    lhs = jnp.concatenate(split(inv_c, 3) + [jnp.zeros((13, n_a * owned), F32)], axis=0).astype(BF16)
    sec = lax.dot_general(lhs, kern, nt, preferred_element_type=F32)
    sec_ref[b] = sec[0:1] + sec[1:2] + sec[2:3]
    for k, peer in enumerate(b_peers):
        send(copy(sec_ref.at[b], sec_ref.at[b], s_s.at[k], s_r.at[b], b_dev(peer)))

    for peer in b_peers:
        copy(rsum_ref.at[b], rsum_ref.at[peer], r_s.at[0], r_r.at[peer], b_dev(peer)).wait_recv()
    inv_r = 1.0 / jnp.sum(rsum_ref[...], axis=0)
    for peer in b_peers:
        copy(sec_ref.at[b], sec_ref.at[peer], s_s.at[0], s_r.at[peer], b_dev(peer)).wait_recv()
    dens = jnp.sum(sec_ref[...], axis=0) * inv_r
    factor = inv_r * lax.rsqrt(dens)
    for i in range(n_b):
        fac_ref[i] = factor[:, i * owned:(i + 1) * owned]
    weighted = (blocks * factor).astype(BF16)
    partial = jnp.dot(weighted, kern, preferred_element_type=F32)
    for i in range(n_a):
        part_ref[i] = partial[:, i * owned:(i + 1) * owned]
    for k, peer in enumerate(a_peers):
        send(copy(part_ref.at[peer], got_ref.at[a], p_s.at[k], p_r.at[a], a_dev(peer)))
    got_ref[a] = part_ref[a]
    for peer in a_peers:
        copy(part_ref.at[a], got_ref.at[peer], p_s.at[0], p_r.at[peer], a_dev(peer)).wait_recv()
    out_ref[...] = jnp.sum(got_ref[...], axis=0) * fac_ref[b]
    for cp in sends:
        cp.wait_send()


def per_device(features, block):
    n_row = lax.axis_size("row")
    n_col = lax.axis_size("col")
    n_y = 2 if n_row % 2 == 0 else 1
    n_a, n_b = n_y * n_col, n_row // n_y
    width, owned = features.shape
    columns = block.shape[0]
    frames = owned * n_row * n_col
    scale = 4.0 / (float(frames) ** (2.0 / width) - 1.0)
    root = math.sqrt(2.0 * math.log2(math.e) / scale)
    lanes = 128 * ((owned + 127) // 128)
    dma = pltpu.SemaphoreType.DMA
    a_sem, b_sem = dma((n_a,)), dma((n_b,))

    def kernel(*refs):
        body(n_a, n_b, n_y, n_col, root, *refs)

    hbm = pl.BlockSpec(memory_space=pltpu.HBM)
    return pl.pallas_call(
        kernel,
        out_shape=pltpu.VMEM(block.shape, F32),
        in_specs=[hbm, hbm],
        out_specs=pl.BlockSpec(memory_space=pltpu.VMEM),
        scratch_shapes=[
            pltpu.VMEM(features.shape, F32),
            pltpu.VMEM((width, lanes), F32),
            pltpu.VMEM((n_b, owned, 128), BF16),
            pltpu.VMEM((n_a, owned, 128), BF16),
            pltpu.VMEM((n_b, columns, owned), F32),
            pltpu.VMEM((n_b, owned, n_a * owned), BF16),
            pltpu.VMEM((n_a, 1, n_a * owned), F32),
            pltpu.VMEM((n_b, 1, n_b * owned), F32),
            pltpu.VMEM((n_b, 1, n_b * owned), F32),
            pltpu.VMEM((n_a, columns, owned), F32),
            pltpu.VMEM((n_a, columns, owned), F32),
            pltpu.VMEM((n_b, 1, owned), F32),
            dma, dma, b_sem, b_sem, a_sem, a_sem, b_sem, b_sem, a_sem, a_sem,
            b_sem, b_sem, b_sem, b_sem, a_sem, a_sem,
        ],
        compiler_params=pltpu.CompilerParams(collective_id=0, has_side_effects=True),
        name="diffusion",
    )(features, block)


def solution(mesh):
    placed = (P(None, ("row", "col")), P(None, ("row", "col")))
    return jax.shard_map(
        per_device, mesh=mesh, in_specs=placed, out_specs=P(None, ("row", "col")), check_vma=False
    )
```

```python
import math

import jax
import jax.numpy as jnp
from jax import lax
from jax.experimental import pallas as pl
from jax.experimental.pallas import tpu as pltpu
from jax.sharding import PartitionSpec as P

F32 = jnp.float32
BF16 = jnp.bfloat16


def split(value, pieces):
    out = []
    for _ in range(pieces):
        piece = value.astype(BF16).astype(F32)
        out.append(piece)
        value = value - piece
    return out


def body(
    n_a, n_b, n_y, n_col, root,
    feat_hbm, block_hbm, out_ref,
    feat_ref, pad_ref, u_ref, v_ref, blk_ref, kern_ref, csum_ref, rsum_ref, sec_ref, part_ref, got_ref, fac_ref,
    f_l, k_l, u_s, u_r, v_s, v_r, k_s, k_r, c_s, c_r, r_s, r_r, s_s, s_r, p_s, p_r,
):
    width, owned = feat_ref.shape
    row, col = lax.axis_index("row"), lax.axis_index("col")
    a = (row % n_y) * n_col + col
    b = row // n_y
    a_peers = [lax.rem(a + k, n_a) for k in range(1, n_a)]
    b_peers = [lax.rem(b + k, n_b) for k in range(1, n_b)]

    def a_dev(peer):
        return (b * n_y + peer // n_col, peer % n_col)

    def b_dev(peer):
        return (peer * n_y + row % n_y, col)

    def copy(src, dst, send, recv, dev):
        return pltpu.make_async_remote_copy(
            src_ref=src, dst_ref=dst, send_sem=send, recv_sem=recv,
            device_id=dev, device_id_type=pl.DeviceIdType.MESH,
        )

    barrier = pltpu.get_barrier_semaphore()
    for peer in a_peers:
        pl.semaphore_signal(barrier, inc=1, device_id=a_dev(peer), device_id_type=pl.DeviceIdType.MESH)
    for peer in b_peers:
        pl.semaphore_signal(barrier, inc=1, device_id=b_dev(peer), device_id_type=pl.DeviceIdType.MESH)

    load = pltpu.make_async_copy(feat_hbm, feat_ref, f_l)
    load.start()
    load_block = pltpu.make_async_copy(block_hbm, blk_ref.at[b], k_l)
    load_block.start()
    pad_ref[...] = jnp.zeros_like(pad_ref)
    load.wait()
    pad_ref[:, :owned] = feat_ref[...] * root
    hi, lo = split(pad_ref[...], 2)
    half = jnp.sum(hi * (0.5 * hi + lo), axis=0, keepdims=True)
    t = [-piece for piece in split(half, 3)]
    one = jnp.ones_like(half)
    zero = jnp.zeros((128 - 3 * width - 6, pad_ref.shape[1]), F32)
    left = jnp.concatenate([hi, lo, hi] + t + [one] * 3 + [zero], axis=0)
    right = jnp.concatenate([hi, hi, lo] + [one] * 3 + t + [zero], axis=0)
    u_ref[b] = left.T[:owned].astype(BF16)
    v_ref[a] = right.T[:owned].astype(BF16)

    pl.semaphore_wait(barrier, n_a + n_b - 2)

    sends = []

    def send(cp):
        cp.start()
        sends.append(cp)

    for k, peer in enumerate(a_peers):
        send(copy(v_ref.at[a], v_ref.at[a], v_s.at[k], v_r.at[a], a_dev(peer)))
    for k, peer in enumerate(b_peers):
        send(copy(u_ref.at[b], u_ref.at[b], u_s.at[k], u_r.at[b], b_dev(peer)))

    for peer in a_peers:
        copy(v_ref.at[a], v_ref.at[peer], v_s.at[0], v_r.at[peer], a_dev(peer)).wait_recv()
    v = v_ref[...].reshape(n_a * owned, 128)

    total = jnp.zeros((8, n_a * owned), F32)
    for peer in [b] + b_peers:
        if peer is not b:
            copy(u_ref.at[b], u_ref.at[peer], u_s.at[0], u_r.at[peer], b_dev(peer)).wait_recv()
        expo = lax.dot_general(u_ref[peer], v, (((1,), (1,)), ((), ())), preferred_element_type=F32)
        tile = jnp.exp2(expo).astype(BF16)
        kern_ref[peer] = tile
        total = total + jnp.sum(tile.astype(F32).reshape(owned // 8, 8, n_a * owned), axis=0)

    csum_ref[a] = jnp.sum(total, axis=0, keepdims=True)
    for k, peer in enumerate(a_peers):
        send(copy(csum_ref.at[a], csum_ref.at[a], c_s.at[k], c_r.at[a], a_dev(peer)))

    load_block.wait()
    for k, peer in enumerate(b_peers):
        send(copy(blk_ref.at[b], blk_ref.at[b], k_s.at[k], k_r.at[b], b_dev(peer)))

    kern = kern_ref[...].reshape(n_b * owned, n_a * owned)
    nt = (((1,), (1,)), ((), ()))
    ones = jnp.ones((16, n_a * owned), BF16)
    rsum_ref[b] = lax.dot_general(ones, kern, nt, preferred_element_type=F32)[:1]
    for k, peer in enumerate(b_peers):
        send(copy(rsum_ref.at[b], rsum_ref.at[b], r_s.at[k], r_r.at[b], b_dev(peer)))

    for peer in a_peers:
        copy(csum_ref.at[a], csum_ref.at[peer], c_s.at[0], c_r.at[peer], a_dev(peer)).wait_recv()
    inv_c = 1.0 / jnp.sum(csum_ref[...], axis=0)
    lhs = jnp.concatenate(split(inv_c, 3) + [jnp.zeros((13, n_a * owned), F32)], axis=0).astype(BF16)
    sec = lax.dot_general(lhs, kern, nt, preferred_element_type=F32)
    sec_ref[b] = sec[0:1] + sec[1:2] + sec[2:3]
    for k, peer in enumerate(b_peers):
        send(copy(sec_ref.at[b], sec_ref.at[b], s_s.at[k], s_r.at[b], b_dev(peer)))

    for peer in b_peers:
        copy(rsum_ref.at[b], rsum_ref.at[peer], r_s.at[0], r_r.at[peer], b_dev(peer)).wait_recv()
    for peer in b_peers:
        copy(blk_ref.at[b], blk_ref.at[peer], k_s.at[0], k_r.at[peer], b_dev(peer)).wait_recv()
    blocks = jnp.concatenate([blk_ref[i] for i in range(n_b)], axis=1)

    inv_r = 1.0 / jnp.sum(rsum_ref[...], axis=0)
    for peer in b_peers:
        copy(sec_ref.at[b], sec_ref.at[peer], s_s.at[0], s_r.at[peer], b_dev(peer)).wait_recv()
    dens = jnp.sum(sec_ref[...], axis=0) * inv_r
    factor = inv_r * lax.rsqrt(dens)
    for i in range(n_b):
        fac_ref[i] = factor[:, i * owned:(i + 1) * owned]
    weighted = (blocks * factor).astype(BF16)
    partial = jnp.dot(weighted, kern, preferred_element_type=F32)
    for i in range(n_a):
        part_ref[i] = partial[:, i * owned:(i + 1) * owned]
    for k, peer in enumerate(a_peers):
        send(copy(part_ref.at[peer], got_ref.at[a], p_s.at[k], p_r.at[a], a_dev(peer)))
    got_ref[a] = part_ref[a]
    for peer in a_peers:
        copy(part_ref.at[a], got_ref.at[peer], p_s.at[0], p_r.at[peer], a_dev(peer)).wait_recv()
    out_ref[...] = jnp.sum(got_ref[...], axis=0) * fac_ref[b]
    for cp in sends:
        cp.wait_send()


def per_device(features, block):
    n_row = lax.axis_size("row")
    n_col = lax.axis_size("col")
    n_y = 2 if n_row % 2 == 0 else 1
    n_a, n_b = n_y * n_col, n_row // n_y
    width, owned = features.shape
    columns = block.shape[0]
    frames = owned * n_row * n_col
    scale = 4.0 / (float(frames) ** (2.0 / width) - 1.0)
    root = math.sqrt(2.0 * math.log2(math.e) / scale)
    lanes = 128 * ((owned + 127) // 128)
    dma = pltpu.SemaphoreType.DMA
    a_sem, b_sem = dma((n_a,)), dma((n_b,))

    def kernel(*refs):
        body(n_a, n_b, n_y, n_col, root, *refs)

    hbm = pl.BlockSpec(memory_space=pltpu.HBM)
    return pl.pallas_call(
        kernel,
        out_shape=pltpu.VMEM(block.shape, F32),
        in_specs=[hbm, hbm],
        out_specs=pl.BlockSpec(memory_space=pltpu.VMEM),
        scratch_shapes=[
            pltpu.VMEM(features.shape, F32),
            pltpu.VMEM((width, lanes), F32),
            pltpu.VMEM((n_b, owned, 128), BF16),
            pltpu.VMEM((n_a, owned, 128), BF16),
            pltpu.VMEM((n_b, columns, owned), F32),
            pltpu.VMEM((n_b, owned, n_a * owned), BF16),
            pltpu.VMEM((n_a, 1, n_a * owned), F32),
            pltpu.VMEM((n_b, 1, n_b * owned), F32),
            pltpu.VMEM((n_b, 1, n_b * owned), F32),
            pltpu.VMEM((n_a, columns, owned), F32),
            pltpu.VMEM((n_a, columns, owned), F32),
            pltpu.VMEM((n_b, 1, owned), F32),
            dma, dma, b_sem, b_sem, a_sem, a_sem, b_sem, b_sem, a_sem, a_sem,
            b_sem, b_sem, b_sem, b_sem, a_sem, a_sem,
        ],
        compiler_params=pltpu.CompilerParams(collective_id=0, has_side_effects=True),
        name="diffusion",
    )(features, block)


def solution(mesh):
    placed = (P(None, ("row", "col")), P(None, ("row", "col")))
    return jax.shard_map(
        per_device, mesh=mesh, in_specs=placed, out_specs=P(None, ("row", "col")), check_vma=False
    )
```

```python
import math

import jax
import jax.numpy as jnp
from jax import lax
from jax.experimental import pallas as pl
from jax.experimental.pallas import tpu as pltpu
from jax.sharding import PartitionSpec as P

F32 = jnp.float32
BF16 = jnp.bfloat16


def split(value, pieces):
    out = []
    for _ in range(pieces):
        piece = value.astype(BF16).astype(F32)
        out.append(piece)
        value = value - piece
    return out


def packable(width, owned):
    spare = 128 - owned
    if spare <= 0 or owned % spare:
        return False
    rest = width * spare // 128
    return rest % 8 == 0 and rest * (owned // spare) == width - rest


def pack(value):
    width, owned = value.shape
    if not packable(width, owned):
        return value
    spare = 128 - owned
    kept = width - width * spare // 128
    rest = [value[kept:, i * spare:(i + 1) * spare] for i in range(owned // spare)]
    return jnp.concatenate([value[:kept], jnp.concatenate(rest, axis=0)], axis=1)


def unpack(value, width, owned):
    if not packable(width, owned):
        return value
    rest = width - value.shape[0]
    parts = [value[i * rest:(i + 1) * rest, owned:] for i in range(value.shape[0] // rest)]
    return jnp.concatenate([value[:, :owned], jnp.concatenate(parts, axis=1)], axis=0)


def operand(value, is_left):
    width = value.shape[0]
    hi, lo = split(value, 2)
    half = jnp.sum(hi * (0.5 * hi + lo), axis=0, keepdims=True)
    t = [-piece for piece in split(half, 3)]
    one = [jnp.ones_like(half)] * 3
    zero = [jnp.zeros((128 - 3 * width - 6, value.shape[1]), F32)]
    parts = [hi, lo, hi] + t + one + zero if is_left else [hi, hi, lo] + one + t + zero
    return jnp.concatenate(parts, axis=0).T.astype(BF16)


def body(
    n_a, n_b, n_y, n_col, root,
    feat_hbm, block_hbm, out_ref,
    feat_ref, x_a, x_b, u_ref, v_ref, blk_ref, kern_ref, csum_ref, rsum_ref, sec_ref, part_ref, got_ref, fac_ref,
    f_l, k_l, u_s, u_r, v_s, v_r, k_s, k_r, c_s, c_r, r_s, r_r, s_s, s_r, p_s, p_r,
):
    width, owned = feat_ref.shape
    row, col = lax.axis_index("row"), lax.axis_index("col")
    a = (row % n_y) * n_col + col
    b = row // n_y
    a_peers = [lax.rem(a + k, n_a) for k in range(1, n_a)]
    b_peers = [lax.rem(b + k, n_b) for k in range(1, n_b)]

    def a_dev(peer):
        return (b * n_y + peer // n_col, peer % n_col)

    def b_dev(peer):
        return (peer * n_y + row % n_y, col)

    def copy(src, dst, send, recv, dev):
        return pltpu.make_async_remote_copy(
            src_ref=src, dst_ref=dst, send_sem=send, recv_sem=recv,
            device_id=dev, device_id_type=pl.DeviceIdType.MESH,
        )

    barrier = pltpu.get_barrier_semaphore()
    for peer in a_peers:
        pl.semaphore_signal(barrier, inc=1, device_id=a_dev(peer), device_id_type=pl.DeviceIdType.MESH)
    for peer in b_peers:
        pl.semaphore_signal(barrier, inc=1, device_id=b_dev(peer), device_id_type=pl.DeviceIdType.MESH)

    load = pltpu.make_async_copy(feat_hbm, feat_ref, f_l)
    load.start()
    load_block = pltpu.make_async_copy(block_hbm, blk_ref.at[b], k_l)
    load_block.start()
    load.wait()
    own = feat_ref[...] * root
    packed = pack(own)
    x_a[a] = packed
    x_b[b] = packed

    pl.semaphore_wait(barrier, n_a + n_b - 2)

    sends = []

    def send(cp):
        cp.start()
        sends.append(cp)

    for k, peer in enumerate(a_peers):
        send(copy(x_a.at[a], x_a.at[a], v_s.at[k], v_r.at[a], a_dev(peer)))
    for k, peer in enumerate(b_peers):
        send(copy(x_b.at[b], x_b.at[b], u_s.at[k], u_r.at[b], b_dev(peer)))

    v_ref[a] = operand(own, False)
    u_ref[b] = operand(own, True)
    for peer in a_peers:
        copy(x_a.at[a], x_a.at[peer], v_s.at[0], v_r.at[peer], a_dev(peer)).wait_recv()
    for peer in a_peers:
        v_ref[peer] = operand(unpack(x_a[peer], width, owned), False)
    v = v_ref[...].reshape(n_a * owned, 128)

    total = jnp.zeros((8, n_a * owned), F32)
    for n, peer in enumerate([b] + b_peers):
        if n == 1:
            for other in b_peers:
                copy(x_b.at[b], x_b.at[other], u_s.at[0], u_r.at[other], b_dev(other)).wait_recv()
            for other in b_peers:
                u_ref[other] = operand(unpack(x_b[other], width, owned), True)
        expo = lax.dot_general(u_ref[peer], v, (((1,), (1,)), ((), ())), preferred_element_type=F32)
        tile = jnp.exp2(expo).astype(BF16)
        kern_ref[peer] = tile
        total = total + jnp.sum(tile.astype(F32).reshape(owned // 8, 8, n_a * owned), axis=0)

    csum_ref[a] = jnp.sum(total, axis=0, keepdims=True)
    for k, peer in enumerate(a_peers):
        send(copy(csum_ref.at[a], csum_ref.at[a], c_s.at[k], c_r.at[a], a_dev(peer)))

    load_block.wait()
    for k, peer in enumerate(b_peers):
        send(copy(blk_ref.at[b], blk_ref.at[b], k_s.at[k], k_r.at[b], b_dev(peer)))

    kern = kern_ref[...].reshape(n_b * owned, n_a * owned)
    nt = (((1,), (1,)), ((), ()))
    ones = jnp.ones((16, n_a * owned), BF16)
    rsum_ref[b] = lax.dot_general(ones, kern, nt, preferred_element_type=F32)[:1]
    for k, peer in enumerate(b_peers):
        send(copy(rsum_ref.at[b], rsum_ref.at[b], r_s.at[k], r_r.at[b], b_dev(peer)))

    for peer in a_peers:
        copy(csum_ref.at[a], csum_ref.at[peer], c_s.at[0], c_r.at[peer], a_dev(peer)).wait_recv()
    inv_c = 1.0 / jnp.sum(csum_ref[...], axis=0)
    lhs = jnp.concatenate(split(inv_c, 3) + [jnp.zeros((13, n_a * owned), F32)], axis=0).astype(BF16)
    sec = lax.dot_general(lhs, kern, nt, preferred_element_type=F32)
    sec_ref[b] = sec[0:1] + sec[1:2] + sec[2:3]
    for k, peer in enumerate(b_peers):
        send(copy(sec_ref.at[b], sec_ref.at[b], s_s.at[k], s_r.at[b], b_dev(peer)))

    for peer in b_peers:
        copy(rsum_ref.at[b], rsum_ref.at[peer], r_s.at[0], r_r.at[peer], b_dev(peer)).wait_recv()
    for peer in b_peers:
        copy(blk_ref.at[b], blk_ref.at[peer], k_s.at[0], k_r.at[peer], b_dev(peer)).wait_recv()
    blocks = jnp.concatenate([blk_ref[i] for i in range(n_b)], axis=1)

    inv_r = 1.0 / jnp.sum(rsum_ref[...], axis=0)
    for peer in b_peers:
        copy(sec_ref.at[b], sec_ref.at[peer], s_s.at[0], s_r.at[peer], b_dev(peer)).wait_recv()
    dens = jnp.sum(sec_ref[...], axis=0) * inv_r
    factor = inv_r * lax.rsqrt(dens)
    for i in range(n_b):
        fac_ref[i] = factor[:, i * owned:(i + 1) * owned]
    weighted = (blocks * factor).astype(BF16)
    partial = jnp.dot(weighted, kern, preferred_element_type=F32)
    for i in range(n_a):
        part_ref[i] = partial[:, i * owned:(i + 1) * owned]
    for k, peer in enumerate(a_peers):
        send(copy(part_ref.at[peer], got_ref.at[a], p_s.at[k], p_r.at[a], a_dev(peer)))
    got_ref[a] = part_ref[a]
    for peer in a_peers:
        copy(part_ref.at[a], got_ref.at[peer], p_s.at[0], p_r.at[peer], a_dev(peer)).wait_recv()
    out_ref[...] = jnp.sum(got_ref[...], axis=0) * fac_ref[b]
    for cp in sends:
        cp.wait_send()


def per_device(features, block):
    n_row = lax.axis_size("row")
    n_col = lax.axis_size("col")
    n_y = 2 if n_row % 2 == 0 else 1
    n_a, n_b = n_y * n_col, n_row // n_y
    width, owned = features.shape
    columns = block.shape[0]
    frames = owned * n_row * n_col
    scale = 4.0 / (float(frames) ** (2.0 / width) - 1.0)
    root = math.sqrt(2.0 * math.log2(math.e) / scale)
    wire = jax.eval_shape(pack, features).shape
    dma = pltpu.SemaphoreType.DMA
    a_sem, b_sem = dma((n_a,)), dma((n_b,))

    def kernel(*refs):
        body(n_a, n_b, n_y, n_col, root, *refs)

    hbm = pl.BlockSpec(memory_space=pltpu.HBM)
    return pl.pallas_call(
        kernel,
        out_shape=pltpu.VMEM(block.shape, F32),
        in_specs=[hbm, hbm],
        out_specs=pl.BlockSpec(memory_space=pltpu.VMEM),
        scratch_shapes=[
            pltpu.VMEM(features.shape, F32),
            pltpu.VMEM((n_a,) + wire, F32),
            pltpu.VMEM((n_b,) + wire, F32),
            pltpu.VMEM((n_b, owned, 128), BF16),
            pltpu.VMEM((n_a, owned, 128), BF16),
            pltpu.VMEM((n_b, columns, owned), F32),
            pltpu.VMEM((n_b, owned, n_a * owned), BF16),
            pltpu.VMEM((n_a, 1, n_a * owned), F32),
            pltpu.VMEM((n_b, 1, n_b * owned), F32),
            pltpu.VMEM((n_b, 1, n_b * owned), F32),
            pltpu.VMEM((n_a, columns, owned), F32),
            pltpu.VMEM((n_a, columns, owned), F32),
            pltpu.VMEM((n_b, 1, owned), F32),
            dma, dma, b_sem, b_sem, a_sem, a_sem, b_sem, b_sem, a_sem, a_sem,
            b_sem, b_sem, b_sem, b_sem, a_sem, a_sem,
        ],
        compiler_params=pltpu.CompilerParams(collective_id=0, has_side_effects=True),
        name="diffusion",
    )(features, block)


def solution(mesh):
    placed = (P(None, ("row", "col")), P(None, ("row", "col")))
    return jax.shard_map(
        per_device, mesh=mesh, in_specs=placed, out_specs=P(None, ("row", "col")), check_vma=False
    )
```

```python
import math

import jax
import jax.numpy as jnp
from jax import lax
from jax.experimental import pallas as pl
from jax.experimental.pallas import tpu as pltpu
from jax.sharding import PartitionSpec as P

F32 = jnp.float32
BF16 = jnp.bfloat16


def split(value, pieces):
    out = []
    for _ in range(pieces):
        piece = value.astype(BF16).astype(F32)
        out.append(piece)
        value = value - piece
    return out


def packable(width, owned):
    spare = 128 - owned
    if spare <= 0 or owned % spare:
        return False
    rest = width * spare // 128
    return rest % 8 == 0 and rest * (owned // spare) == width - rest


def pack(value):
    width, owned = value.shape
    if not packable(width, owned):
        return value
    spare = 128 - owned
    kept = width - width * spare // 128
    rest = [value[kept:, i * spare:(i + 1) * spare] for i in range(owned // spare)]
    return jnp.concatenate([value[:kept], jnp.concatenate(rest, axis=0)], axis=1)


def unpack(value, width, owned):
    if not packable(width, owned):
        return value
    rest = width - value.shape[0]
    parts = [value[i * rest:(i + 1) * rest, owned:] for i in range(value.shape[0] // rest)]
    return jnp.concatenate([value[:, :owned], jnp.concatenate(parts, axis=1)], axis=0)


def operand(value, is_left):
    width = value.shape[0]
    hi, lo = split(value, 2)
    half = jnp.sum(hi * (0.5 * hi + lo), axis=0, keepdims=True)
    t = [-piece for piece in split(half, 3)]
    one = [jnp.ones_like(half)] * 3
    zero = [jnp.zeros((128 - 3 * width - 6, value.shape[1]), F32)]
    parts = [hi, lo, hi] + t + one + zero if is_left else [hi, hi, lo] + one + t + zero
    return jnp.concatenate(parts, axis=0).T.astype(BF16)


def body(
    n_a, n_b, n_y, n_col, root,
    feat_hbm, block_hbm, out_ref,
    feat_ref, x_a, x_b, u_ref, v_ref, blk_ref, kern_ref, csum_ref, rsum_ref, sec_ref, part_ref, got_ref, fac_ref,
    f_l, k_l, u_s, u_r, v_s, v_r, k_s, k_r, c_s, c_r, r_s, r_r, s_s, s_r, p_s, p_r,
):
    width, owned = feat_ref.shape
    row, col = lax.axis_index("row"), lax.axis_index("col")
    a = (row % n_y) * n_col + col
    b = row // n_y
    a_peers = [lax.rem(a + k, n_a) for k in range(1, n_a)]
    b_peers = [lax.rem(b + k, n_b) for k in range(1, n_b)]

    def a_dev(peer):
        return (b * n_y + peer // n_col, peer % n_col)

    def b_dev(peer):
        return (peer * n_y + row % n_y, col)

    def copy(src, dst, send, recv, dev):
        return pltpu.make_async_remote_copy(
            src_ref=src, dst_ref=dst, send_sem=send, recv_sem=recv,
            device_id=dev, device_id_type=pl.DeviceIdType.MESH,
        )

    barrier = pltpu.get_barrier_semaphore()
    for peer in a_peers:
        pl.semaphore_signal(barrier, inc=1, device_id=a_dev(peer), device_id_type=pl.DeviceIdType.MESH)
    for peer in b_peers:
        pl.semaphore_signal(barrier, inc=1, device_id=b_dev(peer), device_id_type=pl.DeviceIdType.MESH)

    load = pltpu.make_async_copy(feat_hbm, feat_ref, f_l)
    load.start()
    load_block = pltpu.make_async_copy(block_hbm, blk_ref.at[b], k_l)
    load_block.start()
    load.wait()
    own = feat_ref[...] * root
    packed = pack(own)
    x_a[a] = packed
    x_b[b] = packed

    pl.semaphore_wait(barrier, n_a + n_b - 2)

    sends = []

    def send(cp):
        cp.start()
        sends.append(cp)

    for k, peer in enumerate(b_peers):
        send(copy(x_b.at[b], x_b.at[b], u_s.at[k], u_r.at[b], b_dev(peer)))
    for k, peer in enumerate(a_peers):
        send(copy(x_a.at[a], x_a.at[a], v_s.at[k], v_r.at[a], a_dev(peer)))

    v_ref[a] = operand(own, False)
    u_ref[b] = operand(own, True)
    for peer in a_peers:
        copy(x_a.at[a], x_a.at[peer], v_s.at[0], v_r.at[peer], a_dev(peer)).wait_recv()
    for peer in a_peers:
        v_ref[peer] = operand(unpack(x_a[peer], width, owned), False)
    v = v_ref[...].reshape(n_a * owned, 128)

    total = jnp.zeros((8, n_a * owned), F32)
    for n, peer in enumerate([b] + b_peers):
        if n == 1:
            for other in b_peers:
                copy(x_b.at[b], x_b.at[other], u_s.at[0], u_r.at[other], b_dev(other)).wait_recv()
            for other in b_peers:
                u_ref[other] = operand(unpack(x_b[other], width, owned), True)
        expo = lax.dot_general(u_ref[peer], v, (((1,), (1,)), ((), ())), preferred_element_type=F32)
        tile = jnp.exp2(expo).astype(BF16)
        kern_ref[peer] = tile
        total = total + jnp.sum(tile.astype(F32).reshape(owned // 8, 8, n_a * owned), axis=0)

    csum_ref[a] = jnp.sum(total, axis=0, keepdims=True)
    for k, peer in enumerate(a_peers):
        send(copy(csum_ref.at[a], csum_ref.at[a], c_s.at[k], c_r.at[a], a_dev(peer)))

    load_block.wait()
    for k, peer in enumerate(b_peers):
        send(copy(blk_ref.at[b], blk_ref.at[b], k_s.at[k], k_r.at[b], b_dev(peer)))

    kern = kern_ref[...].reshape(n_b * owned, n_a * owned)
    nt = (((1,), (1,)), ((), ()))
    ones = jnp.ones((16, n_a * owned), BF16)
    rsum_ref[b] = lax.dot_general(ones, kern, nt, preferred_element_type=F32)[:1]
    for k, peer in enumerate(b_peers):
        send(copy(rsum_ref.at[b], rsum_ref.at[b], r_s.at[k], r_r.at[b], b_dev(peer)))

    for peer in a_peers:
        copy(csum_ref.at[a], csum_ref.at[peer], c_s.at[0], c_r.at[peer], a_dev(peer)).wait_recv()
    inv_c = 1.0 / jnp.sum(csum_ref[...], axis=0)
    lhs = jnp.concatenate(split(inv_c, 3) + [jnp.zeros((13, n_a * owned), F32)], axis=0).astype(BF16)
    sec = lax.dot_general(lhs, kern, nt, preferred_element_type=F32)
    sec_ref[b] = sec[0:1] + sec[1:2] + sec[2:3]
    for k, peer in enumerate(b_peers):
        send(copy(sec_ref.at[b], sec_ref.at[b], s_s.at[k], s_r.at[b], b_dev(peer)))

    for peer in b_peers:
        copy(rsum_ref.at[b], rsum_ref.at[peer], r_s.at[0], r_r.at[peer], b_dev(peer)).wait_recv()
    for peer in b_peers:
        copy(blk_ref.at[b], blk_ref.at[peer], k_s.at[0], k_r.at[peer], b_dev(peer)).wait_recv()
    blocks = jnp.concatenate([blk_ref[i] for i in range(n_b)], axis=1)

    inv_r = 1.0 / jnp.sum(rsum_ref[...], axis=0)
    for peer in b_peers:
        copy(sec_ref.at[b], sec_ref.at[peer], s_s.at[0], s_r.at[peer], b_dev(peer)).wait_recv()
    dens = jnp.sum(sec_ref[...], axis=0) * inv_r
    factor = inv_r * lax.rsqrt(dens)
    for i in range(n_b):
        fac_ref[i] = factor[:, i * owned:(i + 1) * owned]
    weighted = (blocks * factor).astype(BF16)
    partial = jnp.dot(weighted, kern, preferred_element_type=F32)
    for i in range(n_a):
        part_ref[i] = partial[:, i * owned:(i + 1) * owned]
    for k, peer in enumerate(a_peers):
        send(copy(part_ref.at[peer], got_ref.at[a], p_s.at[k], p_r.at[a], a_dev(peer)))
    got_ref[a] = part_ref[a]
    for peer in a_peers:
        copy(part_ref.at[a], got_ref.at[peer], p_s.at[0], p_r.at[peer], a_dev(peer)).wait_recv()
    out_ref[...] = jnp.sum(got_ref[...], axis=0) * fac_ref[b]
    for cp in sends:
        cp.wait_send()


def per_device(features, block):
    n_row = lax.axis_size("row")
    n_col = lax.axis_size("col")
    n_y = 2 if n_row % 2 == 0 else 1
    n_a, n_b = n_y * n_col, n_row // n_y
    width, owned = features.shape
    columns = block.shape[0]
    frames = owned * n_row * n_col
    scale = 4.0 / (float(frames) ** (2.0 / width) - 1.0)
    root = math.sqrt(2.0 * math.log2(math.e) / scale)
    wire = jax.eval_shape(pack, features).shape
    dma = pltpu.SemaphoreType.DMA
    a_sem, b_sem = dma((n_a,)), dma((n_b,))

    def kernel(*refs):
        body(n_a, n_b, n_y, n_col, root, *refs)

    hbm = pl.BlockSpec(memory_space=pltpu.HBM)
    return pl.pallas_call(
        kernel,
        out_shape=pltpu.VMEM(block.shape, F32),
        in_specs=[hbm, hbm],
        out_specs=pl.BlockSpec(memory_space=pltpu.VMEM),
        scratch_shapes=[
            pltpu.VMEM(features.shape, F32),
            pltpu.VMEM((n_a,) + wire, F32),
            pltpu.VMEM((n_b,) + wire, F32),
            pltpu.VMEM((n_b, owned, 128), BF16),
            pltpu.VMEM((n_a, owned, 128), BF16),
            pltpu.VMEM((n_b, columns, owned), F32),
            pltpu.VMEM((n_b, owned, n_a * owned), BF16),
            pltpu.VMEM((n_a, 1, n_a * owned), F32),
            pltpu.VMEM((n_b, 1, n_b * owned), F32),
            pltpu.VMEM((n_b, 1, n_b * owned), F32),
            pltpu.VMEM((n_a, columns, owned), F32),
            pltpu.VMEM((n_a, columns, owned), F32),
            pltpu.VMEM((n_b, 1, owned), F32),
            dma, dma, b_sem, b_sem, a_sem, a_sem, b_sem, b_sem, a_sem, a_sem,
            b_sem, b_sem, b_sem, b_sem, a_sem, a_sem,
        ],
        compiler_params=pltpu.CompilerParams(collective_id=0, has_side_effects=True),
        name="diffusion",
    )(features, block)


def solution(mesh):
    placed = (P(None, ("row", "col")), P(None, ("row", "col")))
    return jax.shard_map(
        per_device, mesh=mesh, in_specs=placed, out_specs=P(None, ("row", "col")), check_vma=False
    )
```
